32 devices in a mesh: aa: 4 (over x, core), ba: 8 (over z, y).
Axes of the slice: x: 2, y: 2, z: 4, core: 2. Of those that a mesh axis runs over, the one named last changes fastest.
Arguments:
- head_outputs: bfloat16 [1024, 4096], P('ba'), may hold values from -6 to 6
- stream: bfloat16 [1024, 4096], P('ba'), may hold values from -6 to 6
- adapter_down_factors: bfloat16 [4096, 512], P(None, 'aa'), may hold values from -0.09375 to 0.09375
- adapter_up_factors: bfloat16 [512, 4096], P('aa'), may hold values from -1.5 to 1.5
- norm_gain_vector: float32 [4096], replicated, may hold values from 0.5 to 1.5
- router_matrix: bfloat16 [4096, 8], replicated, may hold values from -0.09375 to 0.09375
- token_adapter_index: int32 [1024], P('ba'), may hold values from 0 to 31
- token_expert_index: int32 [1024, 2], P('ba'), may hold values from 0 to 7, all different within a row; in each aligned block of 128 rows (0 to 127, 128 to 255, ...) at most 48 rows name the same one
- gate_weight: bfloat16 [8, 4096, 14336], P('ba', None, 'aa'), may hold values from -0.09375 to 0.09375
- up_weight: bfloat16 [8, 4096, 14336], P('ba', None, 'aa'), may hold values from -0.09375 to 0.09375
- down_weight: bfloat16 [8, 14336, 4096], P('ba', 'aa'), may hold values from -0.046875 to 0.046875
Outputs:
- mixed: bfloat16 [1024, 4096], P('ba', 'aa')
- adapter_load: float32 [32], P('aa')
The draws below stay inside these ranges and needn't reach their ends.
Inputs may be any that keep to these rules, and one draw needn't show every extreme that they name: `token_expert_index`: the two experts of a row differ; in each aligned block of 128 rows no expert is named by more than 48 rows.
All inputs are finite; a program needn't handle non-finite values.
Results may differ from the reference program's by a relative error of at most 0.0049.
Values may be sent and summed in bfloat16 or wider, within the bound.
A program may use at most 192 MiB of HBM per device.

```python
import math
import jax
import jax.numpy as jnp
import numpy as np
from jax import lax

MODEL_DIM = 4096
FF = 14336
E = 8
ADAPTER_RANK = 16
TOK_DEV = 128
CAP = 48
TOKENS = 1024
ADAPTER_COUNT = 32
SLOTS = 8
SLOT_FF = 14336
N_BA = 8


def plant(drawn, stream_key, smallest, top_value):
    longest = drawn.shape.index(max(drawn.shape))
    spots = []
    for shift in (0, 1):
        where = [jax.random.randint(jax.random.fold_in(stream_key, axis), (), 0, length) for axis, length in enumerate(drawn.shape)]
        where[longest] = (where[longest] + shift) % drawn.shape[longest]
        spots.append(tuple(where))
    return drawn.at[spots[0]].set(smallest).at[spots[1]].set(top_value)


def shard_levels(rng, shape, split, smallest, high):
    factor_of = 1.0
    for dim, shards_of in split:
        heights = jax.random.uniform(jax.random.fold_in(jax.random.fold_in(rng, 6), dim), (shards_of,), jnp.float32, smallest / len(split), high / len(split))
        factor_of = factor_of * jnp.repeat(jnp.exp(heights), shape[dim] // shards_of).reshape((-1,) + (1,) * (len(shape) - 1 - dim))
    return factor_of


def rank_bounds(count, lean):
    loads = [(1 << 20) // math.isqrt(rank ** lean) + 1 for rank in range(1, count + 1)]
    deviation = 1 + sum(loads) // (1 << 30)
    return np.cumsum(np.array([max(1, weight // deviation) for weight in loads]))


def skewed_ids(own_key, extent, amount, slope):
    table = rank_bounds(amount, slope)
    lot = jax.random.randint(jax.random.fold_in(own_key, 1), extent, 0, int(table[amount - 1]))
    rank = jnp.searchsorted(jnp.asarray(table, jnp.int32), lot, side="right")
    return jax.random.permutation(jax.random.fold_in(own_key, 2), amount)[rank].astype(jnp.int32)


def deal_out(stream_key, own, number, rows, count, top, most, skew):
    sequence = jax.random.permutation(stream_key, count)
    heavy_load, ordinary = portions_of(count, rows * top, most, skew, True), portions_of(count, rows * top, most, skew, False)
    places = jnp.arange(count)

    def named(lengths, turn):
        used = int((lengths > 0).sum())
        fixed = max(1, used // 4)
        shifted = fixed + (places - fixed + turn * (used - fixed)) % max(1, count - fixed)
        return jnp.zeros((count,), jnp.int32).at[sequence[jnp.where(places < fixed, places, shifted)]].set(jnp.asarray(lengths, jnp.int32))

    lengths = jnp.where(number % 4 == 0, named(heavy_load, number // 4), named(ordinary, number - number // 4 - 1))
    mixed = jax.random.permutation(jax.random.fold_in(own, 3), count)
    giver, taker = mixed[0:count // 2 * 2:2], mixed[1:count // 2 * 2:2]
    margin = jnp.minimum(lengths[giver] - 1, most - lengths[taker]) // 2
    margin = jnp.where((giver == sequence[0]) | (taker == sequence[0]) | (lengths[taker] == 0), 0, jnp.maximum(margin, 0))
    shifted = jax.random.randint(jax.random.fold_in(own, 4), (count // 2,), 0, 1 << 20) % (margin + 1)
    lengths = lengths.at[giver].add(-shifted).at[taker].add(shifted)
    labels = jnp.searchsorted(jnp.cumsum(lengths), jnp.arange(rows * top), side="right").astype(jnp.int32)
    table = labels.reshape(top, rows).T
    table = table[jax.random.permutation(jax.random.fold_in(own, 1), rows)]
    turn = jax.random.randint(jax.random.fold_in(own, 2), (rows, 1), 0, top)
    return jnp.take_along_axis(table, (jnp.arange(top)[None, :] + turn) % top, axis=1)


def portions_of(amount, total, most, slope, full):
    portions = [(1 << 20) // math.isqrt(rank ** slope) + 1 for rank in range(1, amount + 1)]
    largest = most if full else min(most, max(-(-total // amount), total * portions[0] // sum(portions)))
    least = 1 if total - largest >= amount - 1 else 0
    counts, spare = [largest] + [least] * (amount - 1), total - largest - least * (amount - 1)
    while spare > 0:
        candidates = [i for i in range(1, amount) if counts[i] < largest] or [i for i in range(1, amount) if counts[i] < most]
        mass, remaining = sum([portions[i] for i in candidates]), spare
        for i in candidates:
            more = min(most - counts[i], max(1, remaining * portions[i] // mass), spare)
            counts[i] = counts[i] + more
            spare = spare - more
    return np.array(counts)


def bell_draw(key, extent, deviation, limit, shards=(), kind=jnp.bfloat16):
    values = jax.random.normal(key, extent, jnp.float32) * deviation
    if len(shards) > 0:
        values = shard_levels(key, extent, shards, -0.22, 0.18) * values
    return jnp.clip(values, min=-limit, max=limit).astype(kind)


def setup_inputs(seed: int = 0) -> dict:
    key_list = jax.random.split(jax.random.key(seed), 12)
    head_outputs = bell_draw(key_list[0], (TOKENS, MODEL_DIM), 1.0, 6.0, ((0, 8),))
    stream = bell_draw(key_list[1], (TOKENS, MODEL_DIM), 1.0, 6.0, ((0, 8),))
    adapter_down_factors = bell_draw(key_list[2], (MODEL_DIM, ADAPTER_COUNT * ADAPTER_RANK), MODEL_DIM ** -0.5, 0.09375, ((1, 4),))
    adapter_up_factors = bell_draw(key_list[3], (ADAPTER_COUNT * ADAPTER_RANK, MODEL_DIM), ADAPTER_RANK ** -0.5, 1.5, ((0, 4),))
    norm_gain_vector = jnp.clip(1.0 + 0.1 * jax.random.normal(key_list[4], (MODEL_DIM,), jnp.float32), 0.5, 1.5)
    router_matrix = bell_draw(key_list[5], (MODEL_DIM, E), MODEL_DIM ** -0.5, 0.09375)
    token_adapter_index = plant(skewed_ids(key_list[6], (TOKENS,), ADAPTER_COUNT, 2), jax.random.fold_in(key_list[6], 3), 0, ADAPTER_COUNT - 1).astype(jnp.int32)
    token_expert_index_keys = jax.random.split(jax.random.fold_in(key_list[7], 1), TOKENS // TOK_DEV)
    token_expert_index_turns = jax.random.permutation(jax.random.fold_in(key_list[7], 3), TOKENS // TOK_DEV)
    token_expert_index = jax.vmap(lambda own, number: deal_out(jax.random.fold_in(key_list[7], 2), own, number, TOK_DEV, E, 2, CAP, 2))(token_expert_index_keys, token_expert_index_turns).reshape((TOKENS, 2))
    gate_weight = bell_draw(key_list[8], (SLOTS, MODEL_DIM, SLOT_FF), MODEL_DIM ** -0.5, 0.09375, ((0, 8), (2, 4)))
    up_weight = bell_draw(key_list[9], (SLOTS, MODEL_DIM, SLOT_FF), MODEL_DIM ** -0.5, 0.09375, ((0, 8), (2, 4)))
    down_weight = bell_draw(key_list[10], (SLOTS, SLOT_FF, MODEL_DIM), FF ** -0.5, 0.046875, ((0, 8), (1, 4)))
    return dict(head_outputs=head_outputs, stream=stream, adapter_down_factors=adapter_down_factors, adapter_up_factors=adapter_up_factors, norm_gain_vector=norm_gain_vector, router_matrix=router_matrix, token_adapter_index=token_adapter_index, token_expert_index=token_expert_index, gate_weight=gate_weight, up_weight=up_weight, down_weight=down_weight)


EPS = 1e-05
ADAPTER_SCALE = 2.0

def reference(head_outputs, stream, adapter_down_factors, adapter_up_factors, norm_gain_vector, router_matrix, token_adapter_index, token_expert_index, gate_weight, up_weight, down_weight):
    rank_projected = jnp.dot(head_outputs, adapter_down_factors, preferred_element_type=jnp.float32)
    column_holder = jnp.arange(adapter_down_factors.shape[1], dtype=jnp.int32) // ADAPTER_RANK
    rank_projected = jnp.where(token_adapter_index[:, None] == column_holder[None, :], rank_projected, 0.0).astype(jnp.bfloat16)
    adapter_update = ADAPTER_SCALE * jnp.dot(rank_projected, adapter_up_factors, preferred_element_type=jnp.float32)
    residual_stream = stream.astype(jnp.float32) + adapter_update
    inv_norm = lax.rsqrt(lax.optimization_barrier(jnp.mean(residual_stream * residual_stream, axis=1, keepdims=True)) + EPS)
    normed = (residual_stream * inv_norm * norm_gain_vector).astype(jnp.bfloat16)
    logits = jnp.dot(normed, router_matrix, preferred_element_type=jnp.float32)
    picked = jnp.take_along_axis(logits, token_expert_index, axis=1)
    weights = 1.0 / (1.0 + jnp.exp(picked[:, ::-1] - picked))
    blocked = token_expert_index.reshape(N_BA, TOK_DEV * 2)
    expert_hits = (blocked[:, :, None] == jnp.arange(E, dtype=jnp.int32)[None, None, :]).astype(jnp.int32)
    before = jnp.cumsum(expert_hits, axis=1) - expert_hits
    position = lax.optimization_barrier(jnp.sum(before * expert_hits, axis=2))
    slot_index = (jnp.arange(N_BA, dtype=jnp.int32)[:, None] * CAP + position).reshape(-1)
    flat_experts = token_expert_index.reshape(-1)
    token_of = jnp.arange(TOKENS * 2, dtype=jnp.int32) // 2
    owner_tok = jnp.zeros((E, N_BA * CAP), jnp.int32).at[flat_experts, slot_index].set(token_of)
    halves = N_BA // E
    results = jnp.zeros((E, N_BA * CAP, normed.shape[1]), jnp.float32)
    for slot_number in range(N_BA):
        expert = slot_number // halves
        slot_rows = normed[owner_tok[expert]]
        gate_proj = jnp.dot(slot_rows, gate_weight[slot_number], preferred_element_type=jnp.float32)
        up_proj = jnp.dot(slot_rows, up_weight[slot_number], preferred_element_type=jnp.float32)
        hidden = (jax.nn.silu(gate_proj) * up_proj).astype(jnp.bfloat16)
        results = results.at[expert].add(jnp.dot(hidden, down_weight[slot_number], preferred_element_type=jnp.float32))
    expert_out = results[flat_experts, slot_index].reshape(TOKENS, 2, -1)
    mixed = residual_stream + lax.optimization_barrier(jnp.sum(weights[:, :, None] * expert_out, axis=1))
    adapter_load = lax.optimization_barrier(jnp.sum((token_adapter_index[:, None] == jnp.arange(ADAPTER_COUNT, dtype=jnp.int32)[None, :]).astype(jnp.float32), axis=0))
    return (mixed.astype(jnp.bfloat16), adapter_load)
```

```python
import functools

import jax
import jax.numpy as jnp
from jax import lax
from jax.experimental import pallas as pl
from jax.experimental.pallas import tpu as pltpu
from jax.sharding import PartitionSpec as P

E = 8
ADAPTER_RANK = 16
CAP = 48
CORES = 2

EPS = 1e-05
ADAPTER_SCALE = 2.0
MESH = pl.DeviceIdType.MESH
F32 = jnp.float32
BF16 = jnp.bfloat16


def cols(block, width):
    return pl.ds(pl.multiple_of(block * width, 128), width)


def greet(places):
    barrier = pltpu.get_barrier_semaphore()
    for place in places:
        pl.semaphore_signal(barrier, inc=1, device_id=place, device_id_type=MESH)
    pl.semaphore_wait(barrier, len(places))


def send(src, dst, send_sem, recv_sem, place):
    copy = pltpu.make_async_remote_copy(
        src_ref=src,
        dst_ref=dst,
        send_sem=send_sem,
        recv_sem=recv_sem,
        device_id=place,
        device_id_type=MESH,
    )
    copy.start()
    return copy


def peers(axis, me, n):
    return [{axis: lax.rem(me + k, n)} for k in range(1, n)]


def front(
    n_aa, n_ba, model_width,
    idx_ref, idxt_ref, head_ref, stream_ref, down_ref, gain_ref, router_ref, up_ref,
    x_ref, res_ref, logit_ref, load_ref,
    up_all, low_all, sq_all, lg_all, ld_all, outgoing,
    own_sem, up_s, up_r, low_s, low_r, sq_s, sq_r, lg_s, lg_r, ld_s, ld_r,
    ba_s, ba_r, xg_s, xg_r, cg_s, cg_r,
):
    aa, ba = lax.axis_index("aa"), lax.axis_index("ba")
    nx = n_aa // CORES
    x, core = aa // CORES, lax.rem(aa, CORES)
    partner = {"aa": x * CORES + 1 - core}
    toks = head_ref.shape[0]
    held = down_ref.shape[1]
    width = model_width // n_aa
    halves = n_ba // E
    aa_peers, ba_peers = peers("aa", aa, n_aa), peers("ba", ba, n_ba)
    greet(aa_peers + ba_peers)
    pending = []

    def fan(places, src, dst, s, r):
        copies = [send(src, dst, s.at[i], r.at[i], p) for i, p in enumerate(places)]
        pending.extend(copies)
        return copies

    up_copies = []
    for k in range(1, n_aa):
        to = lax.rem(aa + k, n_aa)
        up_copies.append(send(
            up_ref.at[:, cols(to, width)], up_all.at[aa], up_s.at[k - 1], up_r.at[k - 1], {"aa": to}
        ))
    pending.extend(up_copies)
    own_up = pltpu.make_async_copy(up_ref.at[:, cols(aa, width)], up_all.at[aa], own_sem)
    own_up.start()

    local = idx_ref[:, 2:3] - aa * (held // ADAPTER_RANK)
    lanes = lax.broadcasted_iota(jnp.int32, (toks, held), 1)
    projected = jnp.dot(head_ref[...], down_ref[...], preferred_element_type=F32)
    low_all[aa] = jnp.where(local == lanes // ADAPTER_RANK, projected, 0.0).astype(BF16)
    low_copies = fan(aa_peers, low_all.at[aa], low_all.at[aa], low_s, low_r)

    tally = jnp.sum((local == lanes).astype(F32), axis=0, keepdims=True)
    ld_all[ba] = jnp.broadcast_to(tally, ld_all.shape[1:])
    ld_copies = fan(ba_peers, ld_all.at[ba], ld_all.at[ba], ld_s, ld_r)

    experts = lax.broadcasted_iota(jnp.int32, (E, toks), 0)
    hits = ((idxt_ref[0:1, :] == experts) | (idxt_ref[1:2, :] == experts)).astype(F32)
    earlier = (
        lax.broadcasted_iota(jnp.int32, (toks, toks), 0)
        < lax.broadcasted_iota(jnp.int32, (toks, toks), 1)
    ).astype(F32)
    place = jnp.dot(hits.astype(BF16), earlier.astype(BF16), preferred_element_type=F32)
    place = jnp.where(hits > 0.0, place, -1.0).astype(jnp.int32)
    spots = lax.broadcasted_iota(jnp.int32, (CAP, toks), 0)

    own_up.wait()
    for copy in low_copies + up_copies:
        copy.wait_recv()
    delta = jnp.dot(low_all[0], up_all[0], preferred_element_type=F32)
    for j in range(1, n_aa):
        delta = delta + jnp.dot(low_all[j], up_all[j], preferred_element_type=F32)
    residual = stream_ref[:, cols(aa, width)].astype(F32) + ADAPTER_SCALE * delta
    res_ref[...] = residual
    square = jnp.sum(residual * residual, axis=1, keepdims=True)
    sq_all[aa] = jnp.broadcast_to(square, sq_all.shape[1:])
    for copy in fan(aa_peers, sq_all.at[aa], sq_all.at[aa], sq_s, sq_r):
        copy.wait_recv()
    total = sq_all[0]
    for j in range(1, n_aa):
        total = total + sq_all[j]
    inv_norm = lax.rsqrt(total[:, 0:1] / model_width + EPS)
    normed = (res_ref[...] * inv_norm * gain_ref[:, cols(aa, width)]).astype(BF16)

    for e in range(E):
        pick = (place[e : e + 1, :] == spots).astype(F32).astype(BF16)
        rows = jnp.dot(pick, normed, preferred_element_type=F32).astype(BF16)
        for j in range(halves):
            outgoing[e * halves + j] = rows
    mine = cols(aa, width)
    ba_copies = []
    for k in range(1, n_ba):
        to = lax.rem(ba + k, n_ba)
        ba_copies.append(send(
            outgoing.at[to], x_ref.at[ba, :, mine], ba_s.at[k - 1], ba_r.at[k - 1], {"ba": to}
        ))
    pending.extend(ba_copies)
    x_ref[ba, :, mine] = outgoing[ba]

    part = jnp.dot(
        normed,
        router_ref[pl.ds(pl.multiple_of(aa * width, 128), width), :],
        preferred_element_type=F32,
    )
    lg_all[aa] = part
    lg_copies = fan(aa_peers, lg_all.at[aa], lg_all.at[aa], lg_s, lg_r)

    x_copies, c_copies = [], []
    for k in range(n_ba):
        source = lax.rem(ba - k + n_ba, n_ba)
        if k:
            ba_copies[k - 1].wait_recv()
        block = x_ref.at[source, :, mine]
        for kx in range(1, nx):
            to = lax.rem(x + kx, nx) * CORES + core
            i = k * (nx - 1) + kx - 1
            x_copies.append(send(block, block, xg_s.at[i], xg_r.at[i], {"aa": to}))
        c_copies.append(send(block, block, cg_s.at[k * nx], cg_r.at[k * nx], partner))
    for k in range(n_ba):
        source = lax.rem(ba - k + n_ba, n_ba)
        for kx in range(1, nx):
            x_copies[k * (nx - 1) + kx - 1].wait_recv()
            origin = lax.rem(x - kx + nx, nx) * CORES + core
            block = x_ref.at[source, :, cols(origin, width)]
            i = k * nx + kx
            c_copies.append(send(block, block, cg_s.at[i], cg_r.at[i], partner))
    pending.extend(x_copies + c_copies)

    for copy in lg_copies + ld_copies:
        copy.wait_recv()
    logits = lg_all[0]
    for j in range(1, n_aa):
        logits = logits + lg_all[j]
    logit_ref[...] = logits
    load = ld_all[0]
    for j in range(1, n_ba):
        load = load + ld_all[j]
    load_ref[...] = load
    for copy in c_copies:
        copy.wait_recv()
    for copy in pending:
        copy.wait_send()


def back(
    n_aa, n_ba,
    idx_ref, res_ref, logit_ref, y_ref,
    out_ref,
    c1, xs, c2, acc, bs, ret,
    c_s, c_r, x_s, x_r, b_s, b_r,
):
    aa, ba = lax.axis_index("aa"), lax.axis_index("ba")
    nx = n_aa // CORES
    x, core = aa // CORES, lax.rem(aa, CORES)
    partner = {"aa": x * CORES + 1 - core}
    toks, width = out_ref.shape
    halves = n_ba // E
    x_peers = [{"aa": lax.rem(x + kx, nx) * CORES + core} for kx in range(1, nx)]
    greet([partner] + x_peers + peers("ba", ba, n_ba))
    order = list(range(1, n_ba)) + [0]
    far_first = list(range(1, nx)) + [0]

    c_copies, x_copies, b_copies = {}, {}, {}
    for k in order:
        to = lax.rem(ba + k, n_ba)
        for kx in far_first:
            block = lax.rem(x + kx, nx) * CORES + 1 - core
            i = k * nx + kx
            c_copies[k, kx] = send(
                y_ref.at[to, :, cols(block, width)], c1.at[kx, k], c_s.at[i], c_r.at[i], partner
            )

    first, second = idx_ref[:, 0:1], idx_ref[:, 1:2]
    experts = lax.broadcasted_iota(jnp.int32, (toks, E), 1)
    hit0, hit1 = (first == experts).astype(F32), (second == experts).astype(F32)
    logits = logit_ref[...]
    own0 = jnp.sum(hit0 * logits, axis=1, keepdims=True)
    own1 = jnp.sum(hit1 * logits, axis=1, keepdims=True)
    weight0 = 1.0 / (1.0 + jnp.exp(own1 - own0))
    weight1 = 1.0 / (1.0 + jnp.exp(own0 - own1))
    earlier = (
        lax.broadcasted_iota(jnp.int32, (toks, toks), 1)
        < lax.broadcasted_iota(jnp.int32, (toks, toks), 0)
    ).astype(F32)
    place = jnp.dot(earlier.astype(BF16), (hit0 + hit1).astype(BF16), preferred_element_type=F32)
    spots = lax.broadcasted_iota(jnp.int32, (toks, n_ba * CAP), 1)

    def picked(expert, hit):
        spot = jnp.sum(hit * place, axis=1, keepdims=True).astype(jnp.int32)
        found = spots == expert * (halves * CAP) + spot
        for j in range(1, halves):
            found = found | (spots == (expert * halves + j) * CAP + spot)
        return found.astype(F32).astype(BF16)

    pick0, pick1 = picked(first, hit0), picked(second, hit1)

    for k in order:
        to = lax.rem(ba + k, n_ba)
        for kx in far_first:
            block = lax.rem(x + kx, nx) * CORES + core
            c_copies[k, kx].wait_recv()
            pair = y_ref[to, :, cols(block, width)].astype(F32) + c1[kx, k].astype(F32)
            if kx:
                i = k * (nx - 1) + kx - 1
                xs[kx - 1, k] = pair.astype(BF16)
                x_copies[k, kx] = send(
                    xs.at[kx - 1, k], c2.at[kx - 1, k], x_s.at[i], x_r.at[i], x_peers[kx - 1]
                )
            else:
                acc[k] = pair
    for k in order:
        total = acc[k]
        for kx in range(1, nx):
            x_copies[k, kx].wait_recv()
            total = total + c2[kx - 1, k].astype(F32)
        if k:
            bs[k - 1] = total.astype(BF16)
            b_copies[k] = send(
                bs.at[k - 1], ret.at[ba], b_s.at[k - 1], b_r.at[k - 1],
                {"ba": lax.rem(ba + k, n_ba)},
            )
        else:
            ret[ba] = total.astype(BF16)
    for k in range(1, n_ba):
        b_copies[k].wait_recv()
    rows = ret[...].reshape(n_ba * CAP, width)
    mixed = weight0 * jnp.dot(pick0, rows, preferred_element_type=F32)
    mixed = mixed + weight1 * jnp.dot(pick1, rows, preferred_element_type=F32)
    out_ref[...] = (res_ref[...] + mixed).astype(BF16)
    for copies in (c_copies, x_copies, b_copies):
        for copy in copies.values():
            copy.wait_send()


def shards(
    head_outputs,
    stream,
    adapter_down_factors,
    adapter_up_factors,
    norm_gain_vector,
    router_matrix,
    token_adapter_index,
    token_expert_index,
    gate_weight,
    up_weight,
    down_weight,
):
    toks, model_width = head_outputs.shape
    n_aa, n_ba = lax.axis_size("aa"), lax.axis_size("ba")
    nx = n_aa // CORES
    held = adapter_down_factors.shape[1]
    width = model_width // n_aa
    vmem = pl.BlockSpec(memory_space=pltpu.VMEM)
    dma = pltpu.SemaphoreType.DMA
    idx = jnp.concatenate([token_expert_index, token_adapter_index[:, None]], axis=1)

    def sems(n):
        return [dma((max(n, 1),)), dma((max(n, 1),))]

    x, residual, logits, load = pl.pallas_call(
        functools.partial(front, n_aa, n_ba, model_width),
        out_shape=(
            jax.ShapeDtypeStruct((n_ba, CAP, model_width), BF16),
            jax.ShapeDtypeStruct((toks, width), F32),
            jax.ShapeDtypeStruct((toks, E), F32),
            jax.ShapeDtypeStruct((8, held), F32),
        ),
        in_specs=[vmem] * 7 + [pl.BlockSpec(memory_space=pl.ANY)],
        out_specs=(vmem,) * 4,
        scratch_shapes=[
            pltpu.VMEM((n_aa, held, width), BF16),
            pltpu.VMEM((n_aa, toks, held), BF16),
            pltpu.VMEM((n_aa, toks, 128), F32),
            pltpu.VMEM((n_aa, toks, E), F32),
            pltpu.VMEM((n_ba, 8, held), F32),
            pltpu.VMEM((n_ba, CAP, width), BF16),
            dma,
        ]
        + sems(n_aa - 1) * 4
        + sems(n_ba - 1) * 2
        + sems(n_ba * (nx - 1))
        + sems(n_ba * nx),
        compiler_params=pltpu.CompilerParams(
            collective_id=0, has_side_effects=True, vmem_limit_bytes=48 * 2**20
        ),
        name="front",
    )(
        idx, token_expert_index.T, head_outputs, stream, adapter_down_factors,
        norm_gain_vector[None, :], router_matrix, adapter_up_factors,
    )
    rows = x.reshape(n_ba * CAP, model_width)
    gate_proj = jnp.dot(rows, gate_weight[0], preferred_element_type=F32)
    up_proj = jnp.dot(rows, up_weight[0], preferred_element_type=F32)
    hidden = (jax.nn.silu(gate_proj) * up_proj).astype(BF16)
    partial_value = jnp.dot(hidden, down_weight[0], preferred_element_type=F32).astype(BF16)
    mixed = pl.pallas_call(
        functools.partial(back, n_aa, n_ba),
        out_shape=jax.ShapeDtypeStruct((toks, width), BF16),
        in_specs=[vmem] * 4,
        out_specs=vmem,
        scratch_shapes=[
            pltpu.VMEM((nx, n_ba, CAP, width), BF16),
            pltpu.VMEM((max(nx - 1, 1), n_ba, CAP, width), BF16),
            pltpu.VMEM((max(nx - 1, 1), n_ba, CAP, width), BF16),
            pltpu.VMEM((n_ba, CAP, width), F32),
            pltpu.VMEM((n_ba - 1, CAP, width), BF16),
            pltpu.VMEM((n_ba, CAP, width), BF16),
        ]
        + sems(n_ba * nx)
        + sems(n_ba * (nx - 1))
        + sems(n_ba - 1),
        compiler_params=pltpu.CompilerParams(
            collective_id=1, has_side_effects=True, vmem_limit_bytes=56 * 2**20
        ),
        name="back",
    )(idx, residual, logits, partial_value.reshape(n_ba, CAP, model_width))
    return (mixed, load[0, : held // ADAPTER_RANK])


def solution(mesh):
    in_specs = (
        P("ba", None),
        P("ba", None),
        P(None, "aa"),
        P("aa", None),
        P(),
        P(),
        P("ba"),
        P("ba", None),
        P("ba", None, "aa"),
        P("ba", None, "aa"),
        P("ba", "aa", None),
    )
    out_specs = (P("ba", "aa"), P("aa"))
    return jax.shard_map(shards, mesh=mesh, in_specs=in_specs, out_specs=out_specs, check_vma=False)
```
